128 devices in a mesh: dp: 64 (over y, x, z), rep: 2 (over core).
Axes of the slice: x: 4, y: 4, z: 4, core: 2. Of those that a mesh axis runs over, the one named last changes fastest.
Arguments:
- row_grads: float32 [65536, 512], P(('dp', 'rep')), may hold values from -2500 to 2500
- token_owner: int32 [65536, 1], P(('dp', 'rep')), may hold values from 0 to 63; in each aligned block of 512 rows (0 to 511, 512 to 1023, ...) at most 16 rows name the same one
- token_row: int32 [65536], P(('dp', 'rep')), may hold values from 0 to 2047
- table: float32 [131072, 512], P('dp'), may hold values from -6 to 6
- moment: float32 [131072, 512], P('dp'), may hold values from -3 to 3
- second: float32 [131072, 512], P('dp'), may hold values from 0.05 to 2
Outputs:
- new_table: float32 [131072, 512], P('dp')
- new_moment: float32 [131072, 512], P('dp')
- new_second: float32 [131072, 512], P('dp')
The draws below stay inside these ranges and needn't reach their ends.
Inputs may be any that keep to these rules, and one draw needn't show every extreme that they name: `token_owner`: among the rows of one device at most 16 name one owner; in every draw some owner is named by exactly 16 rows of some device.
All inputs are finite; a program needn't handle non-finite values.
Results may differ from the reference program's by a relative error of at most 0.00007.
Values sent between devices are 32-bit elements; how exact they have to be, the bound alone decides.
A program may use at most 128 MiB of HBM per device.

```python
import math
import jax
import jax.numpy as jnp
import numpy as np

VOCAB = 131072
ADAM_STEP = 100
TOK_DEV = 512
LW = 512
TOKENS = 65536
ROWS_OWN = 2048
CAP = 16
N_DP = 64
N_REP = 2


def draw_row_grads(key, part):
    keys = jax.random.split(key, 5)
    row_scale = jnp.exp(jax.random.uniform(keys[0], (TOKENS, 1), jnp.float32, 0.0, math.log(10.0)))
    col_scale = jnp.exp(jax.random.uniform(keys[1], (1, LW), jnp.float32, 0.0, math.log(10.0)))
    device_pos = (jnp.arange(TOKENS) // TOK_DEV).astype(jnp.float32)
    ramp = (1.0 + 2.0 * device_pos / max(N_DP * N_REP - 1, 1))[:, None]
    base = jnp.clip(jax.random.normal(keys[4], (TOKENS, LW), jnp.float32), -4.0, 4.0)
    return (base * row_scale * col_scale * ramp).astype(jnp.float32)


def place_ends(drawn, key, least, top_value):
    shape = drawn.shape
    spot = [jax.random.randint(jax.random.fold_in(key, axis), (), 0, shape[axis]) for axis in range(len(shape))]
    drawn = drawn.at[tuple(spot)].set(least)
    longest = shape.index(max(shape))
    spot[longest] = (spot[longest] + 1) % shape[longest]
    return drawn.at[tuple(spot)].set(top_value)


def steps_of(stream_key, shape, shards, least, top_value):
    loudness, own = 1.0, jax.random.fold_in(stream_key, 6)
    for axis_at, blocks in shards:
        heights = jnp.exp(jax.random.uniform(jax.random.fold_in(own, axis_at), (blocks,), jnp.float32, least / len(shards), top_value / len(shards)))
        loudness = loudness * jnp.repeat(heights, shape[axis_at] // blocks).reshape([-1 if axis == axis_at else 1 for axis in range(len(shape))])
    return loudness


def cumulative_ranks(number_of, slope):
    portions = [(1 << 20) // math.isqrt(grade ** slope) + 1 for grade in range(1, number_of + 1)]
    spread = 1 + sum(portions) // (1 << 30)
    return np.cumsum(np.array([max(1, weight // spread) for weight in portions]))


def skewed_ids(rng, shape, amount, lean):
    grid = cumulative_ranks(amount, lean)
    lot = jax.random.randint(jax.random.fold_in(rng, 1), shape, 0, int(grid[amount - 1]))
    grade = jnp.searchsorted(jnp.asarray(grid, jnp.int32), lot, side="right")
    return jax.random.permutation(jax.random.fold_in(rng, 2), amount)[grade].astype(jnp.int32)


def deal_out(stream_key, own, number, rows, count, top, most, lean):
    order = jax.random.permutation(stream_key, count)
    packed, usual = load_shares(count, rows * top, most, lean, True), load_shares(count, rows * top, most, lean, False)
    places = jnp.arange(count)

    def named(lengths, rotation):
        used = int((lengths > 0).sum())
        fixed = max(1, used // 4)
        moved = fixed + (places - fixed + rotation * (used - fixed)) % max(1, count - fixed)
        return jnp.zeros((count,), jnp.int32).at[order[jnp.where(places < fixed, places, moved)]].set(jnp.asarray(lengths, jnp.int32))

    lengths = jnp.where(number % 4 == 0, named(packed, number // 4), named(usual, number - number // 4 - 1))
    mixed = jax.random.permutation(jax.random.fold_in(own, 3), count)
    source_of, sink = mixed[0:count // 2 * 2:2], mixed[1:count // 2 * 2:2]
    slack = jnp.minimum(lengths[source_of] - 1, most - lengths[sink]) // 2
    slack = jnp.where((source_of == order[0]) | (sink == order[0]) | (lengths[sink] == 0), 0, jnp.maximum(slack, 0))
    moved = jax.random.randint(jax.random.fold_in(own, 4), (count // 2,), 0, 1 << 20) % (slack + 1)
    lengths = lengths.at[source_of].add(-moved).at[sink].add(moved)
    labels = jnp.searchsorted(jnp.cumsum(lengths), jnp.arange(rows * top), side="right").astype(jnp.int32)
    grid = labels.reshape(top, rows).T
    grid = grid[jax.random.permutation(jax.random.fold_in(own, 1), rows)]
    rotation = jax.random.randint(jax.random.fold_in(own, 2), (rows, 1), 0, top)
    return jnp.take_along_axis(grid, (jnp.arange(top)[None, :] + rotation) % top, axis=1)


def load_shares(amount, total, most, slope, full):
    weights = [(1 << 20) // math.isqrt(rank ** slope) + 1 for rank in range(1, amount + 1)]
    largest = most if full else min(most, max(-(-total // amount), total * weights[0] // sum(weights)))
    least = 1 if total - largest >= amount - 1 else 0
    holding, spare = [largest] + [least] * (amount - 1), total - largest - least * (amount - 1)
    while spare > 0:
        movable = [i for i in range(1, amount) if holding[i] < largest] or [i for i in range(1, amount) if holding[i] < most]
        pool, budget = sum([weights[i] for i in movable]), spare
        for i in movable:
            extra = min(most - holding[i], max(1, budget * weights[i] // pool), spare)
            holding[i] = holding[i] + extra
            spare = spare - extra
    return np.array(holding)


def noise(rng, dims, deviation, bound, pieces=(), kind=jnp.bfloat16):
    drawn = deviation * jax.random.normal(rng, dims, jnp.float32)
    if pieces:
        drawn = drawn * steps_of(rng, dims, pieces, -0.22, 0.18)
    return jnp.clip(drawn, -bound, bound).astype(kind)


def setup_inputs(seed: int = 0) -> dict:
    splits = jax.random.split(jax.random.key(seed), 7)
    row_grads = draw_row_grads(jax.random.fold_in(splits[6], 71), 0)
    token_owner_keys = jax.random.split(jax.random.fold_in(splits[1], 1), TOKENS // TOK_DEV)
    token_owner_turns = jax.random.permutation(jax.random.fold_in(splits[1], 3), TOKENS // TOK_DEV)
    token_owner = jax.vmap(lambda own, number: deal_out(jax.random.fold_in(splits[1], 2), own, number, TOK_DEV, N_DP, 1, CAP, 2))(token_owner_keys, token_owner_turns).reshape((TOKENS, 1))
    token_row = place_ends(skewed_ids(splits[2], (TOKENS,), ROWS_OWN, 2), jax.random.fold_in(splits[2], 3), 0, ROWS_OWN - 1).astype(jnp.int32)
    table = noise(splits[3], (VOCAB, LW), 1.0, 6.0, ((0, 64),), jnp.float32)
    moment = noise(splits[4], (VOCAB, LW), 0.5, 3.0, ((0, 64),), jnp.float32)
    second = jnp.clip(jnp.exp(math.log(2.0) - 3.6888794 * jax.random.uniform(splits[5], (VOCAB, LW), jnp.float32) ** steps_of(splits[5], (VOCAB, LW), ((0, 64),), -0.2, 0.2)), 0.05, 2.0)
    return {"row_grads": row_grads, "token_owner": token_owner, "token_row": token_row, "table": table, "moment": moment, "second": second}


def reference(row_grads, token_owner, token_row, table, moment, second):
    row_id = (token_owner[:, 0] * ROWS_OWN + token_row).astype(jnp.int32)
    dense = jnp.zeros((VOCAB, LW), jnp.float32).at[row_id].add(row_grads.astype(jnp.float32))
    norm = jnp.sqrt(jnp.sum(dense * dense))
    limit = 0.5 * jnp.sqrt(jnp.float32(VOCAB * LW))
    clip = jnp.minimum(jnp.float32(1.0), limit / (norm + 1e-06))
    clipped = clip * dense
    new_moment = 0.9 * moment + 0.1 * clipped
    new_second = 0.999 * second + 0.001 * clipped * clipped
    first_fix = 1.0 - 0.9 ** ADAM_STEP
    second_fix = 1.0 - 0.999 ** ADAM_STEP
    update = new_moment / first_fix / (jnp.sqrt(new_second / second_fix) + 1e-08)
    new_table = table - 0.01 * (update + 0.01 * table)
    return (new_table, new_moment, new_second)
```

```python
import functools

import jax
import jax.numpy as jnp
from jax import lax
from jax.experimental import pallas as pl
from jax.experimental.pallas import tpu as pltpu
from jax.sharding import PartitionSpec as P

VOCAB = 131072
ADAM_STEP = 100
LW = 512
OWNERS = 64
CAP = 16
ROWS = 2048
TOK = 512
HALF = 256
STEP = 27
MESH = pl.DeviceIdType.MESH
F32 = jnp.float32
BF16 = jnp.bfloat16


def two_parts(value):
    high = value.astype(BF16)
    return high, (value - high.astype(F32)).astype(BF16)


def iota(shape, axis):
    return lax.broadcasted_iota(jnp.int32, shape, axis)


def onehot(mask):
    return jnp.where(mask, 1.0, 0.0).astype(BF16)


def exchange_kernel(
    owner_hbm, row_hbm, grads_hbm, table_hbm, moment_hbm, second_hbm,
    dense, table_out, moment_out, second_out, clip_out,
    owner_ref, row_ref, grads, send, recv, ids_send, ids_recv, ids_own, ids_other, part, parts,
    load_sem, state_sem, ids_sem, ids_got, swap_sem, swap_got,
    send_sem, recv_sem, part_sem, part_got, half_sem, half_got,
):
    me = lax.axis_index("dp")
    core = lax.axis_index("rep")
    y, x, z = me // 16, (me // 4) % 4, me % 4

    def ahead(offset):
        oy, ox, oz = offset // 16, (offset // 4) % 4, offset % 4
        return ((y + oy) % 4) * 16 + ((x + ox) % 4) * 4 + (z + oz) % 4

    loads = [
        pltpu.make_async_copy(source, target, load_sem.at[k])
        for k, (source, target) in enumerate(
            ((owner_hbm, owner_ref), (row_hbm, row_ref), (grads_hbm, grads))
        )
    ]
    for load in loads:
        load.start()
    barrier = pltpu.get_barrier_semaphore()
    for offset in range(1, OWNERS):
        for flip in range(2):
            pl.semaphore_signal(
                barrier, inc=1, device_id=(ahead(offset), (core + flip) % 2), device_id_type=MESH
            )
    pl.semaphore_signal(barrier, inc=1, device_id=(me, 1 - core), device_id_type=MESH)
    states = [
        pltpu.make_async_copy(source, target, state_sem.at[k])
        for k, (source, target) in enumerate(
            ((table_hbm, table_out), (moment_hbm, moment_out), (second_hbm, second_out))
        )
    ]
    for state in states:
        state.start()

    loads[0].wait()
    loads[1].wait()
    owner = owner_ref[...]
    hits = iota((OWNERS, TOK), 0) == owner
    before = onehot(iota((TOK, TOK), 0) < iota((TOK, TOK), 1))
    earlier = jnp.dot(onehot(hits), before, preferred_element_type=F32)
    rank = jnp.sum(jnp.where(hits, earlier, 0.0), axis=0, keepdims=True)
    slot = owner.astype(F32) * float(CAP) + rank

    row = row_ref[...]
    row_high = (row // 64).astype(F32)
    row_low = (row % 64).astype(F32)
    spread = onehot((iota((128, TOK), 0) % CAP).astype(F32) == rank)
    contract = (((1,), (1,)), ((), ()))
    ids = 64.0 * lax.dot_general(
        jnp.where(hits, row_high, 0.0).astype(BF16), spread, contract, preferred_element_type=F32
    ) + lax.dot_general(
        jnp.where(hits, row_low, 0.0).astype(BF16), spread, contract, preferred_element_type=F32
    )
    ids_send[...] = ids.reshape(OWNERS, 1, 128)

    loads[2].wait()
    grads_parts = jnp.concatenate(two_parts(grads[...]), axis=0)

    def place(block, carry):
        pick = onehot((iota((256, TOK), 0) + block * 256).astype(F32) == slot)
        rows = jnp.dot(
            jnp.concatenate((pick, pick), axis=1), grads_parts, preferred_element_type=F32
        )
        send[pl.ds(block * 16, 16), 0] = rows[:, :HALF].reshape(16, CAP, HALF)
        send[pl.ds(block * 16, 16), 1] = rows[:, HALF:].reshape(16, CAP, HALF)
        return carry

    lax.fori_loop(0, 4, place, 0)

    def clear(block, carry):
        dense[core, pl.ds(block * 256, 256)] = jnp.zeros((256, HALF), F32)
        return carry

    lax.fori_loop(0, ROWS // 256, clear, 0)
    recv[119] = send[me, core]
    ids_recv[63] = ids_send[me]

    pl.semaphore_wait(barrier, 127)

    def send_ids(j, carry):
        target = ahead(((j + 1) * STEP) % OWNERS)
        pltpu.make_async_remote_copy(
            ids_send.at[target], ids_recv.at[j], ids_sem, ids_got,
            device_id=(target, core), device_id_type=MESH,
        ).start()
        return carry

    lax.fori_loop(0, 63, send_ids, 0)

    def send_rows(j, carry):
        target = ahead(((j + 1) * STEP) % OWNERS)
        place_at = (j // 8) * 16 + j % 8
        for flip in range(2):
            half = (core + flip) % 2
            pltpu.make_async_remote_copy(
                send.at[target, half], recv.at[place_at + 8 * flip], send_sem,
                recv_sem.at[j // 8], device_id=(target, half), device_id_type=MESH,
            ).start()
        return carry

    lax.fori_loop(0, 63, send_rows, 0)
    pltpu.make_async_remote_copy(
        send.at[me, 1 - core], recv.at[127], send_sem, recv_sem.at[7],
        device_id=(me, 1 - core), device_id_type=MESH,
    ).start()

    pltpu.make_async_copy(ids_recv.at[pl.ds(0, 63)], ids_recv.at[pl.ds(0, 63)], ids_got).wait()
    got = ids_recv[...].reshape(8, 8, 128)
    keep = iota((8, 8, 128), 2) // CAP == iota((8, 8, 128), 1)
    ids_own[...] = jnp.sum(jnp.where(keep, got, 0.0), axis=1)
    swap = pltpu.make_async_remote_copy(
        ids_own, ids_other, swap_sem, swap_got, device_id=(me, 1 - core), device_id_type=MESH
    )
    swap.start()
    swap.wait_recv()

    def gather(group):
        near = ids_own[pl.ds(group, 1), :]
        far = ids_other[pl.ds(group, 1), :]
        ids_here = jnp.concatenate((near, far), axis=1)
        values = jnp.concatenate(
            two_parts(recv[pl.ds(group * 16, 16)].reshape(256, HALF)), axis=0
        )

        def rows_block(block, carry):
            pick = onehot((iota((512, 256), 0) + block * 512).astype(F32) == ids_here)
            dense[core, pl.ds(block * 512, 512)] += jnp.dot(
                jnp.concatenate((pick, pick), axis=1), values, preferred_element_type=F32
            )
            return carry

        lax.fori_loop(0, ROWS // 512, rows_block, 0)

    def group_step(group, carry):
        here = recv.at[pl.ds(group * 16, 16)]
        pltpu.make_async_copy(here, here, recv_sem.at[group]).wait()
        gather(group)
        return carry

    lax.fori_loop(0, 7, group_step, 0)
    last = recv.at[pl.ds(112, 15)]
    pltpu.make_async_copy(last, last, recv_sem.at[7]).wait()
    gather(7)

    def square(block, carry):
        value = dense[core, pl.ds(block * 64, 64)]
        return carry + jnp.sum((value * value).reshape(8, 8, HALF), axis=0)

    squares = lax.fori_loop(0, ROWS // 64, square, jnp.zeros((8, HALF), F32))
    squares = jnp.sum(squares[:, :128] + squares[:, 128:], axis=0, keepdims=True)
    part[...] = squares
    parts[core] = squares
    half_copy = pltpu.make_async_remote_copy(
        dense.at[core], dense.at[core], half_sem, half_got,
        device_id=(me, 1 - core), device_id_type=MESH,
    )
    for offset in [42, *(o for o in range(1, OWNERS) if o != 42)]:
        for flip in range(2):
            pltpu.make_async_remote_copy(
                part, parts.at[2 * offset + core], part_sem, part_got,
                device_id=(ahead(offset), (core + flip) % 2), device_id_type=MESH,
            ).start()
    pltpu.make_async_remote_copy(
        part, parts.at[core], part_sem, part_got,
        device_id=(me, 1 - core), device_id_type=MESH,
    ).start()
    half_copy.start()
    for state in states:
        state.wait()
    swap.wait_send()
    pltpu.make_async_copy(ids_send.at[pl.ds(0, 63)], ids_send.at[pl.ds(0, 63)], ids_sem).wait()
    sent = recv.at[pl.ds(0, 127)]
    pltpu.make_async_copy(sent, sent, send_sem).wait()
    row_count = parts.at[pl.ds(0, 127)]
    pltpu.make_async_copy(row_count, row_count, part_got).wait()
    total = jnp.sum(jnp.sum(parts[...], axis=0), axis=1, keepdims=True)
    limit = 0.5 * jnp.sqrt(jnp.float32(VOCAB * LW))
    scaling = jnp.minimum(1.0, limit / (jnp.sqrt(total) + 1e-06))
    clip_out[...] = jnp.broadcast_to(scaling, (8, 128))
    half_copy.wait()
    pltpu.make_async_copy(row_count, row_count, part_sem).wait()


def exchange(row_grads, token_owner, token_row, table, moment, second):
    vmem = pl.BlockSpec(memory_space=pltpu.VMEM)
    hbm = pl.BlockSpec(memory_space=pl.ANY)
    dma = pltpu.SemaphoreType.DMA
    state = pltpu.VMEM((ROWS, LW), F32)
    return pl.pallas_call(
        exchange_kernel,
        out_shape=(pltpu.VMEM((2, ROWS, HALF), F32), state, state, state, pltpu.VMEM((8, 128), F32)),
        in_specs=[hbm] * 6,
        out_specs=(vmem,) * 5,
        scratch_shapes=[
            pltpu.VMEM((1, TOK), jnp.int32),
            pltpu.VMEM((1, TOK), jnp.int32),
            pltpu.VMEM((TOK, LW), F32),
            pltpu.VMEM((OWNERS, 2, CAP, HALF), F32),
            pltpu.VMEM((128, CAP, HALF), F32),
            pltpu.VMEM((OWNERS, 1, 128), F32),
            pltpu.VMEM((OWNERS, 1, 128), F32),
            pltpu.VMEM((8, 128), F32),
            pltpu.VMEM((8, 128), F32),
            pltpu.VMEM((1, 128), F32),
            pltpu.VMEM((128, 1, 128), F32),
            dma((3,)), dma((3,)), dma, dma, dma, dma, dma, dma((8,)), dma, dma, dma, dma,
        ],
        compiler_params=pltpu.CompilerParams(
            collective_id=0, has_side_effects=True, vmem_limit_bytes=24 * 2**20
        ),
        name="exchange",
    )(
        *(
            pltpu.with_memory_space_constraint(value, pltpu.HBM)
            for value in (
                token_owner.reshape(1, TOK),
                token_row.reshape(1, TOK),
                row_grads,
                table,
                moment,
                second,
            )
        ),
    )


BLOCK = 128
PIECE = 32


def update_kernel(
    dense, table, moment, second, clip,
    table_hbm, moment_hbm, second_hbm,
    table_out, moment_out, second_out, sems,
):
    scaling = jnp.concatenate((clip[...], clip[...]), axis=1)[:1]
    first_fix = 1.0 / (1.0 - 0.9**ADAM_STEP)
    second_fix = 1.0 / (1.0 - 0.999**ADAM_STEP)
    pairs = (
        (table_out, table_hbm),
        (moment_out, moment_hbm),
        (second_out, second_hbm),
    )

    def block_step(block, carry):
        def piece_step(piece, inner):
            rows = pl.ds(pl.multiple_of(block * BLOCK + piece * PIECE, PIECE), PIECE)
            for half in range(2):
                cols = pl.ds(half * HALF, HALF)
                grad = scaling * dense[half, rows, :]
                new_moment = 0.9 * moment[rows, cols] + 0.1 * grad
                new_second = 0.999 * second[rows, cols] + 0.001 * grad * grad
                update = (new_moment * first_fix) / (jnp.sqrt(new_second * second_fix) + 1e-08)
                old = table[rows, cols]
                table_out[rows, cols] = old - 0.01 * (update + 0.01 * old)
                moment_out[rows, cols] = new_moment
                second_out[rows, cols] = new_second
            return inner

        lax.fori_loop(0, BLOCK // PIECE, piece_step, 0)
        span = pl.ds(pl.multiple_of(block * BLOCK, BLOCK), BLOCK)
        for k, (source, target) in enumerate(pairs):
            pltpu.make_async_copy(source.at[span], target.at[span], sems.at[k]).start()
        return carry

    lax.fori_loop(0, ROWS // BLOCK, block_step, 0)
    for k, (source, target) in enumerate(pairs):
        pltpu.make_async_copy(source, target, sems.at[k]).wait()


def update(dense, table, moment, second, clip):
    vmem = pl.BlockSpec(memory_space=pltpu.VMEM)
    hbm = pl.BlockSpec(memory_space=pl.ANY)
    out = jax.ShapeDtypeStruct((ROWS, LW), F32)
    args = [
        pltpu.with_memory_space_constraint(value, pltpu.VMEM)
        for value in (dense, table, moment, second, clip)
    ]
    return pl.pallas_call(
        update_kernel,
        out_shape=(out, out, out),
        in_specs=[vmem] * 5,
        out_specs=(hbm,) * 3,
        scratch_shapes=[pltpu.VMEM((ROWS, LW), F32)] * 3 + [pltpu.SemaphoreType.DMA((3,))],
        compiler_params=pltpu.CompilerParams(vmem_limit_bytes=32 * 2**20),
        name="update",
    )(*args)


def local(row_grads, token_owner, token_row, table, moment, second):
    return update(*exchange(row_grads, token_owner, token_row, table, moment, second))


def solution(mesh):
    return jax.shard_map(
        local,
        mesh=mesh,
        in_specs=(
            P(("dp", "rep"), None),
            P(("dp", "rep"), None),
            P(("dp", "rep")),
            P("dp", None),
            P("dp", None),
            P("dp", None),
        ),
        out_specs=(P("dp", None), P("dp", None), P("dp", None)),
        check_vma=False,
    )
```

```python
import functools

import jax
import jax.numpy as jnp
from jax import lax
from jax.experimental import pallas as pl
from jax.experimental.pallas import tpu as pltpu
from jax.sharding import PartitionSpec as P

VOCAB = 131072
ADAM_STEP = 100
LW = 512
OWNERS = 64
CAP = 16
ROWS = 2048
TOK = 512
HALF = 256
MESH = pl.DeviceIdType.MESH
F32 = jnp.float32
BF16 = jnp.bfloat16


def hops(offset):
    return [min(step, 4 - step) for step in (offset // 16, (offset // 4) % 4, offset % 4)]


def opposite(offset):
    oy, ox, oz = offset // 16, (offset // 4) % 4, offset % 4
    return (-oy % 4) * 16 + (-ox % 4) * 4 + -oz % 4


def turned(offset):
    return (offset % 16) * 4 + offset // 16


def balanced(offsets):
    order = []
    for start in sorted(offsets, key=lambda offset: (-sum(hops(offset)), offset)):
        offset = start
        for _ in range(3):
            for member in (offset, opposite(offset)):
                if member not in order:
                    order.append(member)
            offset = turned(offset)
    return order


FAR_FIRST = balanced(range(1, OWNERS))


def two_parts(value):
    high = value.astype(BF16)
    return high, (value - high.astype(F32)).astype(BF16)


def iota(shape, axis):
    return lax.broadcasted_iota(jnp.int32, shape, axis)


def onehot(mask):
    return jnp.where(mask, 1.0, 0.0).astype(BF16)


def exchange_kernel(
    owner_hbm, row_hbm, grads_hbm, table_hbm, moment_hbm, second_hbm,
    dense, table_out, moment_out, second_out, clip_out,
    owner_ref, row_ref, grads, send, recv, ids_send, ids_recv, ids_own, ids_other, part, parts,
    load_sem, state_sem, ids_sem, ids_got, swap_sem, swap_got,
    send_sem, recv_sem, part_sem, part_got, half_sem, half_got,
):
    me = lax.axis_index("dp")
    core = lax.axis_index("rep")
    y, x, z = me // 16, (me // 4) % 4, me % 4

    def ahead(offset):
        oy, ox, oz = offset // 16, (offset // 4) % 4, offset % 4
        return ((y + oy) % 4) * 16 + ((x + ox) % 4) * 4 + (z + oz) % 4

    loads = [
        pltpu.make_async_copy(source, target, load_sem.at[k])
        for k, (source, target) in enumerate(
            ((owner_hbm, owner_ref), (row_hbm, row_ref), (grads_hbm, grads))
        )
    ]
    for load in loads:
        load.start()
    barrier = pltpu.get_barrier_semaphore()
    for offset in FAR_FIRST:
        for flip in range(2):
            pl.semaphore_signal(
                barrier, inc=1, device_id=(ahead(offset), (core + flip) % 2), device_id_type=MESH
            )
    pl.semaphore_signal(barrier, inc=1, device_id=(me, 1 - core), device_id_type=MESH)
    states = [
        pltpu.make_async_copy(source, target, state_sem.at[k])
        for k, (source, target) in enumerate(
            ((table_hbm, table_out), (moment_hbm, moment_out), (second_hbm, second_out))
        )
    ]
    for state in states:
        state.start()

    loads[0].wait()
    loads[1].wait()
    owner = owner_ref[...]
    hits = iota((OWNERS, TOK), 0) == owner
    before = onehot(iota((TOK, TOK), 0) < iota((TOK, TOK), 1))
    earlier = jnp.dot(onehot(hits), before, preferred_element_type=F32)
    rank = jnp.sum(jnp.where(hits, earlier, 0.0), axis=0, keepdims=True)
    slot = owner.astype(F32) * float(CAP) + rank

    row = row_ref[...]
    row_high = (row // 64).astype(F32)
    row_low = (row % 64).astype(F32)
    spread = onehot((iota((128, TOK), 0) % CAP).astype(F32) == rank)
    contract = (((1,), (1,)), ((), ()))
    ids = 64.0 * lax.dot_general(
        jnp.where(hits, row_high, 0.0).astype(BF16), spread, contract, preferred_element_type=F32
    ) + lax.dot_general(
        jnp.where(hits, row_low, 0.0).astype(BF16), spread, contract, preferred_element_type=F32
    )
    ids_send[...] = ids.reshape(OWNERS, 1, 128)

    loads[2].wait()
    grads_parts = jnp.concatenate(two_parts(grads[...]), axis=0)

    def place(block, carry):
        pick = onehot((iota((256, TOK), 0) + block * 256).astype(F32) == slot)
        rows = jnp.dot(
            jnp.concatenate((pick, pick), axis=1), grads_parts, preferred_element_type=F32
        )
        send[pl.ds(block * 16, 16), 0] = rows[:, :HALF].reshape(16, CAP, HALF)
        send[pl.ds(block * 16, 16), 1] = rows[:, HALF:].reshape(16, CAP, HALF)
        return carry

    lax.fori_loop(0, 4, place, 0)

    def clear(block, carry):
        dense[core, pl.ds(block * 256, 256)] = jnp.zeros((256, HALF), F32)
        return carry

    lax.fori_loop(0, ROWS // 256, clear, 0)
    recv[119] = send[me, core]
    ids_recv[63] = ids_send[me]

    pl.semaphore_wait(barrier, 127)

    for j, offset in enumerate(FAR_FIRST):
        target = ahead(offset)
        pltpu.make_async_remote_copy(
            ids_send.at[target], ids_recv.at[j], ids_sem, ids_got,
            device_id=(target, core), device_id_type=MESH,
        ).start()
    for j, offset in enumerate(FAR_FIRST):
        target = ahead(offset)
        for flip in range(2):
            half = (core + flip) % 2
            pltpu.make_async_remote_copy(
                send.at[target, half], recv.at[(j // 8) * 16 + j % 8 + 8 * flip], send_sem,
                recv_sem.at[j // 8], device_id=(target, half), device_id_type=MESH,
            ).start()
    pltpu.make_async_remote_copy(
        send.at[me, 1 - core], recv.at[127], send_sem, recv_sem.at[7],
        device_id=(me, 1 - core), device_id_type=MESH,
    ).start()

    pltpu.make_async_copy(ids_recv.at[pl.ds(0, 63)], ids_recv.at[pl.ds(0, 63)], ids_got).wait()
    got = ids_recv[...].reshape(8, 8, 128)
    keep = iota((8, 8, 128), 2) // CAP == iota((8, 8, 128), 1)
    ids_own[...] = jnp.sum(jnp.where(keep, got, 0.0), axis=1)
    swap = pltpu.make_async_remote_copy(
        ids_own, ids_other, swap_sem, swap_got, device_id=(me, 1 - core), device_id_type=MESH
    )
    swap.start()
    swap.wait_recv()

    def gather(group, squares=None):
        near = ids_own[pl.ds(group, 1), :]
        far = ids_other[pl.ds(group, 1), :]
        ids_here = jnp.concatenate((near, far), axis=1)
        values = jnp.concatenate(
            two_parts(recv[pl.ds(group * 16, 16)].reshape(256, HALF)), axis=0
        )

        def rows_block(block, carry):
            pick = onehot((iota((1024, 256), 0) + block * 1024).astype(F32) == ids_here)
            rows = pl.ds(block * 1024, 1024)
            total = dense[core, rows] + jnp.dot(
                jnp.concatenate((pick, pick), axis=1), values, preferred_element_type=F32
            )
            dense[core, rows] = total
            if squares is None:
                return carry
            return carry + jnp.sum((total * total).reshape(128, 8, HALF), axis=0)

        return lax.fori_loop(0, ROWS // 1024, rows_block, 0 if squares is None else squares)

    def group_step(group, carry):
        here = recv.at[pl.ds(group * 16, 16)]
        pltpu.make_async_copy(here, here, recv_sem.at[group]).wait()
        gather(group)
        return carry

    lax.fori_loop(0, 7, group_step, 0)
    last = recv.at[pl.ds(112, 15)]
    pltpu.make_async_copy(last, last, recv_sem.at[7]).wait()
    squares = gather(7, jnp.zeros((8, HALF), F32))
    squares = jnp.sum(squares[:, :128] + squares[:, 128:], axis=0, keepdims=True)
    part[...] = squares
    parts[core] = squares
    half_copy = pltpu.make_async_remote_copy(
        dense.at[core], dense.at[core], half_sem, half_got,
        device_id=(me, 1 - core), device_id_type=MESH,
    )
    for offset in FAR_FIRST:
        for flip in range(2):
            pltpu.make_async_remote_copy(
                part, parts.at[2 * offset + core], part_sem, part_got,
                device_id=(ahead(offset), (core + flip) % 2), device_id_type=MESH,
            ).start()
    pltpu.make_async_remote_copy(
        part, parts.at[core], part_sem, part_got,
        device_id=(me, 1 - core), device_id_type=MESH,
    ).start()
    half_copy.start()
    for state in states:
        state.wait()
    swap.wait_send()
    pltpu.make_async_copy(ids_send.at[pl.ds(0, 63)], ids_send.at[pl.ds(0, 63)], ids_sem).wait()
    sent = recv.at[pl.ds(0, 127)]
    pltpu.make_async_copy(sent, sent, send_sem).wait()
    row_count = parts.at[pl.ds(0, 127)]
    pltpu.make_async_copy(row_count, row_count, part_got).wait()
    total = jnp.sum(jnp.sum(parts[...], axis=0), axis=1, keepdims=True)
    limit = 0.5 * jnp.sqrt(jnp.float32(VOCAB * LW))
    scaling = jnp.minimum(1.0, limit / (jnp.sqrt(total) + 1e-06))
    clip_out[...] = jnp.broadcast_to(scaling, (8, 128))
    half_copy.wait()
    pltpu.make_async_copy(row_count, row_count, part_sem).wait()


def exchange(row_grads, token_owner, token_row, table, moment, second):
    vmem = pl.BlockSpec(memory_space=pltpu.VMEM)
    hbm = pl.BlockSpec(memory_space=pl.ANY)
    dma = pltpu.SemaphoreType.DMA
    state = pltpu.VMEM((ROWS, LW), F32)
    return pl.pallas_call(
        exchange_kernel,
        out_shape=(pltpu.VMEM((2, ROWS, HALF), F32), state, state, state, pltpu.VMEM((8, 128), F32)),
        in_specs=[hbm] * 6,
        out_specs=(vmem,) * 5,
        scratch_shapes=[
            pltpu.VMEM((1, TOK), jnp.int32),
            pltpu.VMEM((1, TOK), jnp.int32),
            pltpu.VMEM((TOK, LW), F32),
            pltpu.VMEM((OWNERS, 2, CAP, HALF), F32),
            pltpu.VMEM((128, CAP, HALF), F32),
            pltpu.VMEM((OWNERS, 1, 128), F32),
            pltpu.VMEM((OWNERS, 1, 128), F32),
            pltpu.VMEM((8, 128), F32),
            pltpu.VMEM((8, 128), F32),
            pltpu.VMEM((1, 128), F32),
            pltpu.VMEM((128, 1, 128), F32),
            dma((3,)), dma((3,)), dma, dma, dma, dma, dma, dma((8,)), dma, dma, dma, dma,
        ],
        compiler_params=pltpu.CompilerParams(
            collective_id=0, has_side_effects=True, vmem_limit_bytes=24 * 2**20
        ),
        name="exchange",
    )(
        *(
            pltpu.with_memory_space_constraint(value, pltpu.HBM)
            for value in (
                token_owner.reshape(1, TOK),
                token_row.reshape(1, TOK),
                row_grads,
                table,
                moment,
                second,
            )
        ),
    )


BLOCK = 128
PIECE = 64


def update_kernel(
    dense, table, moment, second, clip,
    table_hbm, moment_hbm, second_hbm,
    table_out, moment_out, second_out, sems,
):
    scaling = jnp.concatenate((clip[...], clip[...]), axis=1)[:1]
    first_fix = 1.0 / (1.0 - 0.9**ADAM_STEP)
    second_fix = 1.0 / (1.0 - 0.999**ADAM_STEP)
    pairs = (
        (table_out, table_hbm),
        (moment_out, moment_hbm),
        (second_out, second_hbm),
    )

    def block_step(block, carry):
        def piece_step(piece, inner):
            rows = pl.ds(pl.multiple_of(block * BLOCK + piece * PIECE, PIECE), PIECE)
            for half in range(2):
                cols = pl.ds(half * HALF, HALF)
                grad = scaling * dense[half, rows, :]
                new_moment = 0.9 * moment[rows, cols] + 0.1 * grad
                new_second = 0.999 * second[rows, cols] + 0.001 * grad * grad
                update = (new_moment * first_fix) / (jnp.sqrt(new_second * second_fix) + 1e-08)
                old = table[rows, cols]
                table_out[rows, cols] = old - 0.01 * (update + 0.01 * old)
                moment_out[rows, cols] = new_moment
                second_out[rows, cols] = new_second
            return inner

        lax.fori_loop(0, BLOCK // PIECE, piece_step, 0)
        span = pl.ds(pl.multiple_of(block * BLOCK, BLOCK), BLOCK)
        for k, (source, target) in enumerate(pairs):
            pltpu.make_async_copy(source.at[span], target.at[span], sems.at[k]).start()
        return carry

    lax.fori_loop(0, ROWS // BLOCK, block_step, 0)
    for k, (source, target) in enumerate(pairs):
        pltpu.make_async_copy(source, target, sems.at[k]).wait()


def update(dense, table, moment, second, clip):
    vmem = pl.BlockSpec(memory_space=pltpu.VMEM)
    hbm = pl.BlockSpec(memory_space=pl.ANY)
    out = jax.ShapeDtypeStruct((ROWS, LW), F32)
    args = [
        pltpu.with_memory_space_constraint(value, pltpu.VMEM)
        for value in (dense, table, moment, second, clip)
    ]
    return pl.pallas_call(
        update_kernel,
        out_shape=(out, out, out),
        in_specs=[vmem] * 5,
        out_specs=(hbm,) * 3,
        scratch_shapes=[pltpu.VMEM((ROWS, LW), F32)] * 3 + [pltpu.SemaphoreType.DMA((3,))],
        compiler_params=pltpu.CompilerParams(vmem_limit_bytes=32 * 2**20),
        name="update",
    )(*args)


def local(row_grads, token_owner, token_row, table, moment, second):
    return update(*exchange(row_grads, token_owner, token_row, table, moment, second))


def solution(mesh):
    return jax.shard_map(
        local,
        mesh=mesh,
        in_specs=(
            P(("dp", "rep"), None),
            P(("dp", "rep"), None),
            P(("dp", "rep")),
            P("dp", None),
            P("dp", None),
            P("dp", None),
        ),
        out_specs=(P("dp", None), P("dp", None), P("dp", None)),
        check_vma=False,
    )
```

```python
import functools

import jax
import jax.numpy as jnp
from jax import lax
from jax.experimental import pallas as pl
from jax.experimental.pallas import tpu as pltpu
from jax.sharding import PartitionSpec as P

VOCAB = 131072
ADAM_STEP = 100
LW = 512
OWNERS = 64
CAP = 16
ROWS = 2048
TOK = 512
HALF = 256
MESH = pl.DeviceIdType.MESH
F32 = jnp.float32
BF16 = jnp.bfloat16


def hops(offset):
    return [min(step, 4 - step) for step in (offset // 16, (offset // 4) % 4, offset % 4)]


def opposite(offset):
    oy, ox, oz = offset // 16, (offset // 4) % 4, offset % 4
    return (-oy % 4) * 16 + (-ox % 4) * 4 + -oz % 4


def turned(offset):
    return (offset % 16) * 4 + offset // 16


def balanced(offsets):
    order = []
    for start in sorted(offsets, key=lambda offset: (-sum(hops(offset)), offset)):
        offset = start
        for _ in range(3):
            for member in (offset, opposite(offset)):
                if member not in order:
                    order.append(member)
            offset = turned(offset)
    return order


FAR_FIRST = balanced(range(1, OWNERS))


def two_parts(value):
    high = value.astype(BF16)
    return high, (value - high.astype(F32)).astype(BF16)


def iota(shape, axis):
    return lax.broadcasted_iota(jnp.int32, shape, axis)


def onehot(mask):
    return jnp.where(mask, 1.0, 0.0).astype(BF16)


def exchange_kernel(
    owner_hbm, row_hbm, grads_hbm, table_hbm, moment_hbm, second_hbm,
    dense, table_out, moment_out, second_out, clip_out,
    owner_ref, row_ref, grads, send, recv, ids_send, ids_recv, ids_own, ids_other, part, parts,
    load_sem, state_sem, ids_sem, ids_got, swap_sem, swap_got,
    send_sem, recv_sem, part_sem, part_got, half_sem, half_got,
):
    me = lax.axis_index("dp")
    core = lax.axis_index("rep")
    y, x, z = me // 16, (me // 4) % 4, me % 4

    def ahead(offset):
        oy, ox, oz = offset // 16, (offset // 4) % 4, offset % 4
        return ((y + oy) % 4) * 16 + ((x + ox) % 4) * 4 + (z + oz) % 4

    loads = [
        pltpu.make_async_copy(source, target, load_sem.at[k])
        for k, (source, target) in enumerate(
            ((owner_hbm, owner_ref), (row_hbm, row_ref), (grads_hbm, grads))
        )
    ]
    for load in loads:
        load.start()
    barrier = pltpu.get_barrier_semaphore()
    for offset in FAR_FIRST:
        for flip in range(2):
            pl.semaphore_signal(
                barrier, inc=1, device_id=(ahead(offset), (core + flip) % 2), device_id_type=MESH
            )
    pl.semaphore_signal(barrier, inc=1, device_id=(me, 1 - core), device_id_type=MESH)
    states = [
        pltpu.make_async_copy(source, target, state_sem.at[k])
        for k, (source, target) in enumerate(
            ((table_hbm, table_out), (moment_hbm, moment_out), (second_hbm, second_out))
        )
    ]
    for state in states:
        state.start()

    loads[0].wait()
    loads[1].wait()
    owner = owner_ref[...]
    hits = iota((OWNERS, TOK), 0) == owner
    before = onehot(iota((TOK, TOK), 0) < iota((TOK, TOK), 1))
    earlier = jnp.dot(onehot(hits), before, preferred_element_type=F32)
    rank = jnp.sum(jnp.where(hits, earlier, 0.0), axis=0, keepdims=True)
    slot = owner.astype(F32) * float(CAP) + rank

    row = row_ref[...]
    row_high = (row // 64).astype(F32)
    row_low = (row % 64).astype(F32)
    spread = onehot((iota((128, TOK), 0) % CAP).astype(F32) == rank)
    contract = (((1,), (1,)), ((), ()))
    ids = 64.0 * lax.dot_general(
        jnp.where(hits, row_high, 0.0).astype(BF16), spread, contract, preferred_element_type=F32
    ) + lax.dot_general(
        jnp.where(hits, row_low, 0.0).astype(BF16), spread, contract, preferred_element_type=F32
    )
    ids_send[...] = ids.reshape(OWNERS, 1, 128)

    loads[2].wait()
    grads_parts = jnp.concatenate(two_parts(grads[...]), axis=0)

    def place(block, carry):
        pick = onehot((iota((256, TOK), 0) + block * 256).astype(F32) == slot)
        rows = jnp.dot(
            jnp.concatenate((pick, pick), axis=1), grads_parts, preferred_element_type=F32
        )
        send[pl.ds(block * 16, 16), 0] = rows[:, :HALF].reshape(16, CAP, HALF)
        send[pl.ds(block * 16, 16), 1] = rows[:, HALF:].reshape(16, CAP, HALF)
        return carry

    lax.fori_loop(0, 4, place, 0)

    def clear(block, carry):
        dense[core, pl.ds(block * 256, 256)] = jnp.zeros((256, HALF), F32)
        return carry

    lax.fori_loop(0, ROWS // 256, clear, 0)
    recv[119] = send[me, core]
    ids_recv[63] = ids_send[me]

    pl.semaphore_wait(barrier, 127)

    for j, offset in enumerate(FAR_FIRST):
        target = ahead(offset)
        pltpu.make_async_remote_copy(
            ids_send.at[target], ids_recv.at[j], ids_sem, ids_got,
            device_id=(target, core), device_id_type=MESH,
        ).start()
    for j, offset in enumerate(FAR_FIRST):
        target = ahead(offset)
        for flip in range(2):
            half = (core + flip) % 2
            pltpu.make_async_remote_copy(
                send.at[target, half], recv.at[(j // 8) * 16 + j % 8 + 8 * flip], send_sem,
                recv_sem.at[j // 8], device_id=(target, half), device_id_type=MESH,
            ).start()
    pltpu.make_async_remote_copy(
        send.at[me, 1 - core], recv.at[127], send_sem, recv_sem.at[7],
        device_id=(me, 1 - core), device_id_type=MESH,
    ).start()

    pltpu.make_async_copy(ids_recv.at[pl.ds(0, 63)], ids_recv.at[pl.ds(0, 63)], ids_got).wait()
    got = ids_recv[...].reshape(8, 8, 128)
    keep = iota((8, 8, 128), 2) // CAP == iota((8, 8, 128), 1)
    ids_own[...] = jnp.sum(jnp.where(keep, got, 0.0), axis=1)
    swap = pltpu.make_async_remote_copy(
        ids_own, ids_other, swap_sem, swap_got, device_id=(me, 1 - core), device_id_type=MESH
    )
    swap.start()
    swap.wait_recv()

    def gather(group):
        near = ids_own[pl.ds(group, 1), :]
        far = ids_other[pl.ds(group, 1), :]
        ids_here = jnp.concatenate((near, far), axis=1)
        values = jnp.concatenate(
            two_parts(recv[pl.ds(group * 16, 16)].reshape(256, HALF)), axis=0
        )

        pick = onehot(iota((ROWS, 256), 0).astype(F32) == ids_here)
        total = dense[core] + jnp.dot(
            jnp.concatenate((pick, pick), axis=1), values, preferred_element_type=F32
        )
        dense[core] = total
        return total

    def group_step(group, carry):
        here = recv.at[pl.ds(group * 16, 16)]
        pltpu.make_async_copy(here, here, recv_sem.at[group]).wait()
        gather(group)
        return carry

    lax.fori_loop(0, 7, group_step, 0)
    last = recv.at[pl.ds(112, 15)]
    pltpu.make_async_copy(last, last, recv_sem.at[7]).wait()
    total = gather(7)
    squares = jnp.sum((total * total).reshape(ROWS // 8, 8, HALF), axis=0)
    squares = jnp.sum(squares[:, :128] + squares[:, 128:], axis=0, keepdims=True)
    part[...] = squares
    parts[core] = squares
    half_copy = pltpu.make_async_remote_copy(
        dense.at[core], dense.at[core], half_sem, half_got,
        device_id=(me, 1 - core), device_id_type=MESH,
    )
    for offset in FAR_FIRST:
        for flip in range(2):
            pltpu.make_async_remote_copy(
                part, parts.at[2 * offset + core], part_sem, part_got,
                device_id=(ahead(offset), (core + flip) % 2), device_id_type=MESH,
            ).start()
    pltpu.make_async_remote_copy(
        part, parts.at[core], part_sem, part_got,
        device_id=(me, 1 - core), device_id_type=MESH,
    ).start()
    half_copy.start()
    for state in states:
        state.wait()
    swap.wait_send()
    pltpu.make_async_copy(ids_send.at[pl.ds(0, 63)], ids_send.at[pl.ds(0, 63)], ids_sem).wait()
    sent = recv.at[pl.ds(0, 127)]
    pltpu.make_async_copy(sent, sent, send_sem).wait()
    row_count = parts.at[pl.ds(0, 127)]
    pltpu.make_async_copy(row_count, row_count, part_got).wait()
    total = jnp.sum(jnp.sum(parts[...], axis=0), axis=1, keepdims=True)
    limit = 0.5 * jnp.sqrt(jnp.float32(VOCAB * LW))
    scaling = jnp.minimum(1.0, limit / (jnp.sqrt(total) + 1e-06))
    clip_out[...] = jnp.broadcast_to(scaling, (8, 128))
    half_copy.wait()
    pltpu.make_async_copy(row_count, row_count, part_sem).wait()


def exchange(row_grads, token_owner, token_row, table, moment, second):
    vmem = pl.BlockSpec(memory_space=pltpu.VMEM)
    hbm = pl.BlockSpec(memory_space=pl.ANY)
    dma = pltpu.SemaphoreType.DMA
    state = pltpu.VMEM((ROWS, LW), F32)
    return pl.pallas_call(
        exchange_kernel,
        out_shape=(pltpu.VMEM((2, ROWS, HALF), F32), state, state, state, pltpu.VMEM((8, 128), F32)),
        in_specs=[hbm] * 6,
        out_specs=(vmem,) * 5,
        scratch_shapes=[
            pltpu.VMEM((1, TOK), jnp.int32),
            pltpu.VMEM((1, TOK), jnp.int32),
            pltpu.VMEM((TOK, LW), F32),
            pltpu.VMEM((OWNERS, 2, CAP, HALF), F32),
            pltpu.VMEM((128, CAP, HALF), F32),
            pltpu.VMEM((OWNERS, 1, 128), F32),
            pltpu.VMEM((OWNERS, 1, 128), F32),
            pltpu.VMEM((8, 128), F32),
            pltpu.VMEM((8, 128), F32),
            pltpu.VMEM((1, 128), F32),
            pltpu.VMEM((128, 1, 128), F32),
            dma((3,)), dma((3,)), dma, dma, dma, dma, dma, dma((8,)), dma, dma, dma, dma,
        ],
        compiler_params=pltpu.CompilerParams(
            collective_id=0, has_side_effects=True, vmem_limit_bytes=24 * 2**20
        ),
        name="exchange",
    )(
        *(
            pltpu.with_memory_space_constraint(value, pltpu.HBM)
            for value in (
                token_owner.reshape(1, TOK),
                token_row.reshape(1, TOK),
                row_grads,
                table,
                moment,
                second,
            )
        ),
    )


BLOCK = 128
PIECE = 64


def update_kernel(
    dense, table, moment, second, clip,
    table_hbm, moment_hbm, second_hbm,
    table_out, moment_out, second_out, sems,
):
    scaling = jnp.concatenate((clip[...], clip[...]), axis=1)[:1]
    first_fix = 1.0 / (1.0 - 0.9**ADAM_STEP)
    second_fix = 1.0 / (1.0 - 0.999**ADAM_STEP)
    pairs = (
        (table_out, table_hbm),
        (moment_out, moment_hbm),
        (second_out, second_hbm),
    )

    def block_step(block, carry):
        def piece_step(piece, inner):
            rows = pl.ds(pl.multiple_of(block * BLOCK + piece * PIECE, PIECE), PIECE)
            for half in range(2):
                cols = pl.ds(half * HALF, HALF)
                grad = scaling * dense[half, rows, :]
                new_moment = 0.9 * moment[rows, cols] + 0.1 * grad
                new_second = 0.999 * second[rows, cols] + 0.001 * grad * grad
                update = (new_moment * first_fix) / (jnp.sqrt(new_second * second_fix) + 1e-08)
                old = table[rows, cols]
                table_out[rows, cols] = old - 0.01 * (update + 0.01 * old)
                moment_out[rows, cols] = new_moment
                second_out[rows, cols] = new_second
            return inner

        lax.fori_loop(0, BLOCK // PIECE, piece_step, 0)
        span = pl.ds(pl.multiple_of(block * BLOCK, BLOCK), BLOCK)
        for k, (source, target) in enumerate(pairs):
            pltpu.make_async_copy(source.at[span], target.at[span], sems.at[k]).start()
        return carry

    lax.fori_loop(0, ROWS // BLOCK, block_step, 0)
    for k, (source, target) in enumerate(pairs):
        pltpu.make_async_copy(source, target, sems.at[k]).wait()


def update(dense, table, moment, second, clip):
    vmem = pl.BlockSpec(memory_space=pltpu.VMEM)
    hbm = pl.BlockSpec(memory_space=pl.ANY)
    out = jax.ShapeDtypeStruct((ROWS, LW), F32)
    args = [
        pltpu.with_memory_space_constraint(value, pltpu.VMEM)
        for value in (dense, table, moment, second, clip)
    ]
    return pl.pallas_call(
        update_kernel,
        out_shape=(out, out, out),
        in_specs=[vmem] * 5,
        out_specs=(hbm,) * 3,
        scratch_shapes=[pltpu.VMEM((ROWS, LW), F32)] * 3 + [pltpu.SemaphoreType.DMA((3,))],
        compiler_params=pltpu.CompilerParams(vmem_limit_bytes=32 * 2**20),
        name="update",
    )(*args)


def local(row_grads, token_owner, token_row, table, moment, second):
    return update(*exchange(row_grads, token_owner, token_row, table, moment, second))


def solution(mesh):
    return jax.shard_map(
        local,
        mesh=mesh,
        in_specs=(
            P(("dp", "rep"), None),
            P(("dp", "rep"), None),
            P(("dp", "rep")),
            P("dp", None),
            P("dp", None),
            P("dp", None),
        ),
        out_specs=(P("dp", None), P("dp", None), P("dp", None)),
        check_vma=False,
    )
```

```python
import functools

import jax
import jax.numpy as jnp
from jax import lax
from jax.experimental import pallas as pl
from jax.experimental.pallas import tpu as pltpu
from jax.sharding import PartitionSpec as P

VOCAB = 131072
ADAM_STEP = 100
LW = 512
OWNERS = 64
CAP = 16
ROWS = 2048
TOK = 512
HALF = 256
MESH = pl.DeviceIdType.MESH
F32 = jnp.float32
BF16 = jnp.bfloat16


def hops(offset):
    return [min(step, 4 - step) for step in (offset // 16, (offset // 4) % 4, offset % 4)]


def opposite(offset):
    oy, ox, oz = offset // 16, (offset // 4) % 4, offset % 4
    return (-oy % 4) * 16 + (-ox % 4) * 4 + -oz % 4


def turned(offset):
    return (offset % 16) * 4 + offset // 16


def balanced(offsets):
    order = []
    for start in sorted(offsets, key=lambda offset: (-sum(hops(offset)), offset)):
        offset = start
        for _ in range(3):
            for member in (offset, opposite(offset)):
                if member not in order:
                    order.append(member)
            offset = turned(offset)
    return order


FAR_FIRST = balanced(range(1, OWNERS))


def two_parts(value):
    high = value.astype(BF16)
    return high, (value - high.astype(F32)).astype(BF16)


def iota(shape, axis):
    return lax.broadcasted_iota(jnp.int32, shape, axis)


def onehot(mask):
    return jnp.where(mask, 1.0, 0.0).astype(BF16)


def exchange_kernel(
    owner_hbm, row_hbm, grads_hbm, table_hbm, moment_hbm, second_hbm,
    dense, table_out, moment_out, second_out, clip_out,
    owner_ref, row_ref, grads, send, recv, ids_send, ids_recv, ids_own, ids_other, part, parts,
    load_sem, state_sem, ids_sem, ids_got, swap_sem, swap_got,
    send_sem, recv_sem, part_sem, part_got, half_sem, half_got,
):
    me = lax.axis_index("dp")
    core = lax.axis_index("rep")
    y, x, z = me // 16, (me // 4) % 4, me % 4

    def ahead(offset):
        oy, ox, oz = offset // 16, (offset // 4) % 4, offset % 4
        return ((y + oy) % 4) * 16 + ((x + ox) % 4) * 4 + (z + oz) % 4

    loads = [
        pltpu.make_async_copy(source, target, load_sem.at[k])
        for k, (source, target) in enumerate(
            ((owner_hbm, owner_ref), (row_hbm, row_ref), (grads_hbm, grads))
        )
    ]
    for load in loads:
        load.start()
    barrier = pltpu.get_barrier_semaphore()
    for offset in FAR_FIRST:
        for flip in range(2):
            pl.semaphore_signal(
                barrier, inc=1, device_id=(ahead(offset), (core + flip) % 2), device_id_type=MESH
            )
    pl.semaphore_signal(barrier, inc=1, device_id=(me, 1 - core), device_id_type=MESH)
    states = [
        pltpu.make_async_copy(source, target, state_sem.at[k])
        for k, (source, target) in enumerate(
            ((table_hbm, table_out), (moment_hbm, moment_out), (second_hbm, second_out))
        )
    ]
    for state in states:
        state.start()

    loads[0].wait()
    loads[1].wait()
    owner = owner_ref[...]
    hits = iota((OWNERS, TOK), 0) == owner
    before = onehot(iota((TOK, TOK), 0) < iota((TOK, TOK), 1))
    earlier = jnp.dot(onehot(hits), before, preferred_element_type=F32)
    rank = jnp.sum(jnp.where(hits, earlier, 0.0), axis=0, keepdims=True)
    slot = owner.astype(F32) * float(CAP) + rank

    row = row_ref[...]
    row_high = (row // 64).astype(F32)
    row_low = (row % 64).astype(F32)
    spread = onehot((iota((128, TOK), 0) % CAP).astype(F32) == rank)
    contract = (((1,), (1,)), ((), ()))
    ids = 64.0 * lax.dot_general(
        jnp.where(hits, row_high, 0.0).astype(BF16), spread, contract, preferred_element_type=F32
    ) + lax.dot_general(
        jnp.where(hits, row_low, 0.0).astype(BF16), spread, contract, preferred_element_type=F32
    )
    ids_send[...] = ids.reshape(OWNERS, 1, 128)

    loads[2].wait()
    grads_parts = jnp.concatenate(two_parts(grads[...]), axis=0)

    def place(block, carry):
        pick = onehot((iota((256, TOK), 0) + block * 256).astype(F32) == slot)
        rows = jnp.dot(
            jnp.concatenate((pick, pick), axis=1), grads_parts, preferred_element_type=F32
        )
        send[pl.ds(block * 16, 16), 0] = rows[:, :HALF].reshape(16, CAP, HALF)
        send[pl.ds(block * 16, 16), 1] = rows[:, HALF:].reshape(16, CAP, HALF)
        return carry

    lax.fori_loop(0, 4, place, 0)

    def clear(block, carry):
        dense[core, pl.ds(block * 256, 256)] = jnp.zeros((256, HALF), F32)
        return carry

    lax.fori_loop(0, ROWS // 256, clear, 0)
    recv[119] = send[me, core]
    ids_recv[63] = ids_send[me]

    pl.semaphore_wait(barrier, 127)

    def send_rows(first, last):
        for j in range(first, last):
            target = ahead(FAR_FIRST[j])
            for flip in range(2):
                half = (core + flip) % 2
                pltpu.make_async_remote_copy(
                    send.at[target, half], recv.at[(j // 8) * 16 + j % 8 + 8 * flip], send_sem,
                    recv_sem.at[j // 8], device_id=(target, half), device_id_type=MESH,
                ).start()

    send_rows(0, 8)
    for j, offset in enumerate(FAR_FIRST):
        target = ahead(offset)
        pltpu.make_async_remote_copy(
            ids_send.at[target], ids_recv.at[j], ids_sem, ids_got,
            device_id=(target, core), device_id_type=MESH,
        ).start()
    send_rows(8, 63)
    pltpu.make_async_remote_copy(
        send.at[me, 1 - core], recv.at[127], send_sem, recv_sem.at[7],
        device_id=(me, 1 - core), device_id_type=MESH,
    ).start()

    pltpu.make_async_copy(ids_recv.at[pl.ds(0, 63)], ids_recv.at[pl.ds(0, 63)], ids_got).wait()
    got = ids_recv[...].reshape(8, 8, 128)
    keep = iota((8, 8, 128), 2) // CAP == iota((8, 8, 128), 1)
    ids_own[...] = jnp.sum(jnp.where(keep, got, 0.0), axis=1)
    swap = pltpu.make_async_remote_copy(
        ids_own, ids_other, swap_sem, swap_got, device_id=(me, 1 - core), device_id_type=MESH
    )
    swap.start()
    swap.wait_recv()

    def gather(group):
        near = ids_own[pl.ds(group, 1), :]
        far = ids_other[pl.ds(group, 1), :]
        ids_here = jnp.concatenate((near, far), axis=1)
        values = jnp.concatenate(
            two_parts(recv[pl.ds(group * 16, 16)].reshape(256, HALF)), axis=0
        )

        pick = onehot(iota((ROWS, 256), 0).astype(F32) == ids_here)
        total = dense[core] + jnp.dot(
            jnp.concatenate((pick, pick), axis=1), values, preferred_element_type=F32
        )
        dense[core] = total
        return total

    def group_step(group, carry):
        here = recv.at[pl.ds(group * 16, 16)]
        pltpu.make_async_copy(here, here, recv_sem.at[group]).wait()
        gather(group)
        return carry

    lax.fori_loop(0, 7, group_step, 0)
    last = recv.at[pl.ds(112, 15)]
    pltpu.make_async_copy(last, last, recv_sem.at[7]).wait()
    total = gather(7)
    squares = jnp.sum((total * total).reshape(ROWS // 8, 8, HALF), axis=0)
    squares = jnp.sum(squares[:, :128] + squares[:, 128:], axis=0, keepdims=True)
    part[...] = squares
    parts[core] = squares
    half_copy = pltpu.make_async_remote_copy(
        dense.at[core], dense.at[core], half_sem, half_got,
        device_id=(me, 1 - core), device_id_type=MESH,
    )
    for offset in FAR_FIRST:
        for flip in range(2):
            pltpu.make_async_remote_copy(
                part, parts.at[2 * offset + core], part_sem, part_got,
                device_id=(ahead(offset), (core + flip) % 2), device_id_type=MESH,
            ).start()
    pltpu.make_async_remote_copy(
        part, parts.at[core], part_sem, part_got,
        device_id=(me, 1 - core), device_id_type=MESH,
    ).start()
    half_copy.start()
    for state in states:
        state.wait()
    swap.wait_send()
    pltpu.make_async_copy(ids_send.at[pl.ds(0, 63)], ids_send.at[pl.ds(0, 63)], ids_sem).wait()
    sent = recv.at[pl.ds(0, 127)]
    pltpu.make_async_copy(sent, sent, send_sem).wait()
    row_count = parts.at[pl.ds(0, 127)]
    pltpu.make_async_copy(row_count, row_count, part_got).wait()
    total = jnp.sum(jnp.sum(parts[...], axis=0), axis=1, keepdims=True)
    limit = 0.5 * jnp.sqrt(jnp.float32(VOCAB * LW))
    scaling = jnp.minimum(1.0, limit / (jnp.sqrt(total) + 1e-06))
    clip_out[...] = jnp.broadcast_to(scaling, (8, 128))
    half_copy.wait()
    pltpu.make_async_copy(row_count, row_count, part_sem).wait()


def exchange(row_grads, token_owner, token_row, table, moment, second):
    vmem = pl.BlockSpec(memory_space=pltpu.VMEM)
    hbm = pl.BlockSpec(memory_space=pl.ANY)
    dma = pltpu.SemaphoreType.DMA
    state = pltpu.VMEM((ROWS, LW), F32)
    return pl.pallas_call(
        exchange_kernel,
        out_shape=(pltpu.VMEM((2, ROWS, HALF), F32), state, state, state, pltpu.VMEM((8, 128), F32)),
        in_specs=[hbm] * 6,
        out_specs=(vmem,) * 5,
        scratch_shapes=[
            pltpu.VMEM((1, TOK), jnp.int32),
            pltpu.VMEM((1, TOK), jnp.int32),
            pltpu.VMEM((TOK, LW), F32),
            pltpu.VMEM((OWNERS, 2, CAP, HALF), F32),
            pltpu.VMEM((128, CAP, HALF), F32),
            pltpu.VMEM((OWNERS, 1, 128), F32),
            pltpu.VMEM((OWNERS, 1, 128), F32),
            pltpu.VMEM((8, 128), F32),
            pltpu.VMEM((8, 128), F32),
            pltpu.VMEM((1, 128), F32),
            pltpu.VMEM((128, 1, 128), F32),
            dma((3,)), dma((3,)), dma, dma, dma, dma, dma, dma((8,)), dma, dma, dma, dma,
        ],
        compiler_params=pltpu.CompilerParams(
            collective_id=0, has_side_effects=True, vmem_limit_bytes=24 * 2**20
        ),
        name="exchange",
    )(
        *(
            pltpu.with_memory_space_constraint(value, pltpu.HBM)
            for value in (
                token_owner.reshape(1, TOK),
                token_row.reshape(1, TOK),
                row_grads,
                table,
                moment,
                second,
            )
        ),
    )


BLOCK = 128
PIECE = 64


def update_kernel(
    dense, table, moment, second, clip,
    table_hbm, moment_hbm, second_hbm,
    table_out, moment_out, second_out, sems,
):
    scaling = jnp.concatenate((clip[...], clip[...]), axis=1)[:1]
    first_fix = 1.0 / (1.0 - 0.9**ADAM_STEP)
    second_fix = 1.0 / (1.0 - 0.999**ADAM_STEP)
    pairs = (
        (table_out, table_hbm),
        (moment_out, moment_hbm),
        (second_out, second_hbm),
    )

    def block_step(block, carry):
        def piece_step(piece, inner):
            rows = pl.ds(pl.multiple_of(block * BLOCK + piece * PIECE, PIECE), PIECE)
            for half in range(2):
                cols = pl.ds(half * HALF, HALF)
                grad = scaling * dense[half, rows, :]
                new_moment = 0.9 * moment[rows, cols] + 0.1 * grad
                new_second = 0.999 * second[rows, cols] + 0.001 * grad * grad
                update = (new_moment * first_fix) / (jnp.sqrt(new_second * second_fix) + 1e-08)
                old = table[rows, cols]
                table_out[rows, cols] = old - 0.01 * (update + 0.01 * old)
                moment_out[rows, cols] = new_moment
                second_out[rows, cols] = new_second
            return inner

        lax.fori_loop(0, BLOCK // PIECE, piece_step, 0)
        span = pl.ds(pl.multiple_of(block * BLOCK, BLOCK), BLOCK)
        for k, (source, target) in enumerate(pairs):
            pltpu.make_async_copy(source.at[span], target.at[span], sems.at[k]).start()
        return carry

    lax.fori_loop(0, ROWS // BLOCK, block_step, 0)
    for k, (source, target) in enumerate(pairs):
        pltpu.make_async_copy(source, target, sems.at[k]).wait()


def update(dense, table, moment, second, clip):
    vmem = pl.BlockSpec(memory_space=pltpu.VMEM)
    hbm = pl.BlockSpec(memory_space=pl.ANY)
    out = jax.ShapeDtypeStruct((ROWS, LW), F32)
    args = [
        pltpu.with_memory_space_constraint(value, pltpu.VMEM)
        for value in (dense, table, moment, second, clip)
    ]
    return pl.pallas_call(
        update_kernel,
        out_shape=(out, out, out),
        in_specs=[vmem] * 5,
        out_specs=(hbm,) * 3,
        scratch_shapes=[pltpu.VMEM((ROWS, LW), F32)] * 3 + [pltpu.SemaphoreType.DMA((3,))],
        compiler_params=pltpu.CompilerParams(vmem_limit_bytes=32 * 2**20),
        name="update",
    )(*args)


def local(row_grads, token_owner, token_row, table, moment, second):
    return update(*exchange(row_grads, token_owner, token_row, table, moment, second))


def solution(mesh):
    return jax.shard_map(
        local,
        mesh=mesh,
        in_specs=(
            P(("dp", "rep"), None),
            P(("dp", "rep"), None),
            P(("dp", "rep")),
            P("dp", None),
            P("dp", None),
            P("dp", None),
        ),
        out_specs=(P("dp", None), P("dp", None), P("dp", None)),
        check_vma=False,
    )
```
